32 devices in a mesh: owner: 4 (over x, core), rows: 8 (over z, y).
Axes of the slice: x: 2, y: 2, z: 4, core: 2. Of those that a mesh axis runs over, the one named last changes fastest.
Arguments:
- master_gate: float32 [64, 2048, 1408], P('owner', 'rows'), may hold values from -0.1875 to 0.1875
- master_up: float32 [64, 2048, 1408], P('owner', 'rows'), may hold values from -0.1875 to 0.1875
- router_weight: float32 [2048, 64], P('rows', 'owner'), may hold values from -0.125 to 0.125
- router_gain: float32 [2048], P('rows'), may hold values from 0.25 to 1.75
Outputs:
- final_gate: bfloat16 [64, 2048, 1408], P('owner', None, 'rows')
- final_up: bfloat16 [64, 2048, 1408], P('owner', None, 'rows')
- scale_gate: float32 [64, 1408], P('owner', 'rows')
- scale_up: float32 [64, 1408], P('owner', 'rows')
- serve_router: bfloat16 [2048, 64], replicated
The draws below stay inside these ranges and needn't reach their ends.
All inputs are finite; a program needn't handle non-finite values. Where the reference program divides by a largest or mean magnitude, that divisor is 1e-20 or more.
Results may differ from the reference program's by a relative error of at most 0.001.
Values may be sent and summed in bfloat16 or wider, within the bound.
No kernel may reach another device: no remote copies, remote signals or barrier semaphores. Data moves between devices by JAX's collectives and lax.ppermute only.
A program may use at most 192 MiB of HBM per device.

```python
import jax
import jax.numpy as jnp

EXPERTS = 64
D_MODEL = 2048
D_EXPERT = 1408


def strengthened(entries, key, source, target, blocks, factor):
    owner, partner = [(jnp.arange(entries.shape[dim]) // (entries.shape[dim] // blocks)).reshape([-1 if axis == dim else 1 for axis in range(entries.ndim)]) for dim in (source, target)]
    chosen = jax.random.permutation(key, blocks)[partner]
    strong = (owner == chosen) | (owner == (partner + blocks // 2) % blocks)
    return jnp.where(strong, factor * entries, entries)


def levels(stream_key, dims, pieces, low, largest):
    level = 1.0
    for position, shards_of in pieces:
        steps = jax.random.uniform(jax.random.fold_in(jax.random.fold_in(stream_key, 6), position), (shards_of,), jnp.float32, low / len(pieces), largest / len(pieces))
        level = level * jnp.repeat(jnp.exp(steps), dims[position] // shards_of).reshape((-1,) + (1,) * (len(dims) - 1 - position))
    return level


def centred(rng, extent, spread, limit, shards=(), dtype=jnp.bfloat16):
    result = spread * jax.random.normal(rng, extent, jnp.float32)
    if shards:
        result = result * levels(rng, extent, shards, -0.22, 0.18)
    return jnp.clip(result, -limit, limit).astype(dtype)


def gaussian_with(own_key, shape, scale, bound, cuts, heavy, dtype=jnp.bfloat16):
    drawn = scale * jax.random.normal(own_key, shape, jnp.float32)
    if cuts:
        drawn = drawn * levels(own_key, shape, cuts, -0.22, 0.18)
    return jnp.clip(strengthened(drawn, jax.random.fold_in(own_key, 3), *heavy), -bound, bound).astype(dtype)


def setup_inputs(seed: int = 0) -> dict:
    streams_of = jax.random.split(jax.random.key(seed), 5)
    return {
        "master_gate": gaussian_with(streams_of[0], (EXPERTS, D_MODEL, D_EXPERT), D_MODEL ** -0.5, 0.1875, ((0, 4), (1, 8)), (1, 2, 8, 2.0), jnp.float32),
        "master_up": gaussian_with(streams_of[1], (EXPERTS, D_MODEL, D_EXPERT), D_MODEL ** -0.5, 0.1875, ((0, 4), (1, 8)), (1, 2, 8, 2.0), jnp.float32),
        "router_weight": centred(streams_of[2], (D_MODEL, EXPERTS), D_MODEL ** -0.5, 0.125, ((0, 8), (1, 4)), jnp.float32),
        "router_gain": jnp.clip(1.0 + 0.15 * jax.random.normal(streams_of[3], (D_MODEL,), jnp.float32), 0.25, 1.75),
    }


def reference(master_gate, master_up, router_weight, router_gain):
    scale_gate = jnp.max(jnp.abs(master_gate), axis=1)
    final_gate = (master_gate / jnp.expand_dims(scale_gate, 1)).astype(jnp.bfloat16)
    scale_up = jnp.max(jnp.abs(master_up), axis=1)
    final_up = (master_up / jnp.expand_dims(scale_up, 1)).astype(jnp.bfloat16)
    serve_router = (router_weight * router_gain[:, None]).astype(jnp.bfloat16)
    return final_gate, final_up, scale_gate, scale_up, serve_router
```

```python
import functools

import jax
import jax.numpy as jnp
from jax import lax
from jax.experimental import pallas as pl
from jax.experimental.pallas import tpu as pltpu
from jax.sharding import PartitionSpec as P


SPAN = 252.0
LN2 = 0.6931471805599453
TINY = 1e-30


def plain_shards(master_gate, master_up, router_weight, router_gain):
    scale_gate, scale_up = lax.pmax(
        (jnp.max(jnp.abs(master_gate), axis=1), jnp.max(jnp.abs(master_up), axis=1)), "rows"
    )
    finals, scales = [], []
    for master, scale in ((master_gate, scale_gate), (master_up, scale_up)):
        narrow = (master / jnp.expand_dims(scale, 1)).astype(jnp.bfloat16)
        final = lax.all_to_all(narrow, "rows", split_axis=2, concat_axis=1, tiled=True)
        width = final.shape[2]
        finals.append(final)
        scales.append(lax.dynamic_slice_in_dim(scale, lax.axis_index("rows") * width, width, axis=1))
    part_router = (router_weight * router_gain[:, None]).astype(jnp.bfloat16)
    row_router = lax.all_gather(part_router, "rows", axis=0, tiled=True)
    serve_router = lax.all_gather(row_router, "owner", axis=1, tiled=True)
    return (*finals, *scales, serve_router)


def pack_body(n, me_ref, x_ref, *refs):
    pieces, top_ref, turned = refs[:n], refs[n], refs[n + 1]
    depth = turned.shape[0]
    width = depth // n
    for c in range(depth // 128):
        cols = slice(128 * c, 128 * (c + 1))
        x = x_ref[0, :, cols]
        size = jnp.abs(x)
        top = jnp.max(size, axis=0, keepdims=True)
        top_ref[0, :, cols] = top
        root = jnp.sqrt(size * (1.0 / jnp.maximum(top, TINY)))
        code = jnp.exp((SPAN * LN2) * root - (SPAN * LN2 / 2))
        code = jnp.where(x < 0, -code, code)
        turned[cols, :] = code.T.astype(jnp.bfloat16)
    for k in range(n):
        to = lax.rem(me_ref[0] + k, n)
        pieces[k][0] = turned[pl.ds(pl.multiple_of(to * width, width), width), :]


def pack(me, master, first, count, n):
    _, rows, depth = master.shape
    width = depth // n
    return pl.pallas_call(
        functools.partial(pack_body, n),
        grid_spec=pltpu.PrefetchScalarGridSpec(
            num_scalar_prefetch=1,
            grid=(count,),
            in_specs=[pl.BlockSpec((1, rows, depth), lambda e, me: (first + e, 0, 0))],
            out_specs=[pl.BlockSpec((1, width, rows), lambda e, me: (e, 0, 0))] * n
            + [pl.BlockSpec((1, 1, depth), lambda e, me: (e, 0, 0))],
            scratch_shapes=[pltpu.VMEM((depth, rows), jnp.bfloat16)],
        ),
        out_shape=[jax.ShapeDtypeStruct((count, width, rows), jnp.bfloat16)] * n
        + [jax.ShapeDtypeStruct((count, 1, depth), jnp.float32)],
        cost_estimate=pl.CostEstimate(
            flops=count * rows * depth * 40, bytes_accessed=count * rows * depth * 6, transcendentals=0
        ),
    )(me, master)


def unpack_body(n, me_ref, ratio_ref, *refs):
    pieces, out = refs[:n], refs[-1]
    width, rows = pieces[0].shape[1:]
    step = 16

    def some_rows(i, _):
        part = pl.ds(pl.multiple_of(i * step, step), step)
        ratio = ratio_ref[0, part, :]
        for k in range(n):
            code = pieces[k][0, part, :].astype(jnp.float32)
            root = jnp.log(jnp.abs(code)) * (1.0 / (SPAN * LN2)) + 0.5
            value = root * root * ratio[:, k : k + 1]
            value = jnp.where(code < 0, -value, value).astype(jnp.bfloat16)
            source = lax.rem(me_ref[0] + (n - k), n)
            out[0, part, pl.ds(pl.multiple_of(source * rows, rows), rows)] = value
        return 0

    lax.fori_loop(0, width // step, some_rows, 0)


def unpack(me, ratio, pieces, whole, first, shape):
    n = len(pieces)
    count, width, rows = pieces[0].shape
    operands = [ratio, *pieces] + ([] if whole is None else [whole])
    return pl.pallas_call(
        functools.partial(unpack_body, n),
        grid_spec=pltpu.PrefetchScalarGridSpec(
            num_scalar_prefetch=1,
            grid=(count,),
            in_specs=[pl.BlockSpec((1, width, n), lambda e, me: (first + e, 0, 0))]
            + [pl.BlockSpec((1, width, rows), lambda e, me: (e, 0, 0))] * n
            + ([] if whole is None else [pl.BlockSpec(memory_space=pl.ANY)]),
            out_specs=pl.BlockSpec((1, width, n * rows), lambda e, me: (first + e, 0, 0)),
        ),
        out_shape=jax.ShapeDtypeStruct(shape, jnp.bfloat16),
        input_output_aliases={} if whole is None else {n + 2: 0},
        cost_estimate=pl.CostEstimate(
            flops=count * rows * width * n * 30, bytes_accessed=count * rows * width * n * 4, transcendentals=0
        ),
    )(me, *operands)


def plan(experts):
    small = max(1, experts // 8)
    return (
        (0, 0, small),
        (0, small, experts - small),
        (1, 0, experts - small),
        (1, experts - small, small),
    )


def join_body(n, me_ref, *refs):
    out, rows = refs[n], refs[0].shape[1]
    for k in range(n):
        source = lax.rem(me_ref[0] + (n - k), n)
        out[:, pl.ds(pl.multiple_of(source * rows, rows), rows)] = refs[k][...]


def join(me, pieces):
    n = len(pieces)
    columns, rows = pieces[0].shape
    return pl.pallas_call(
        functools.partial(join_body, n),
        in_specs=[pl.BlockSpec(memory_space=pltpu.SMEM)] + [pl.BlockSpec(memory_space=pltpu.VMEM)] * n,
        out_specs=pl.BlockSpec(memory_space=pltpu.VMEM),
        out_shape=jax.ShapeDtypeStruct((columns, n * rows), jnp.bfloat16),
        name="join",
    )(me, *pieces)


def send_order(n):
    return sorted(range(1, n), key=lambda k: abs(2 * k - n))


def fast_shards(n, masters, router_weight, router_gain):
    me = lax.axis_index("rows")
    here = jnp.reshape(me, (1,)).astype(jnp.int32)
    experts, rows, depth = masters[0].shape
    width = depth // n
    turns = [[(r, (r + k) % n) for r in range(n)] for k in range(n)]

    def send(pieces):
        came = list(pieces)
        for k in send_order(n):
            came[k] = lax.ppermute(pieces[k], "rows", turns[k])
        return came

    chunks = plan(experts)
    packed, tops = [], [[], []]
    for a, first, count in chunks:
        *pieces, top = pack(here, masters[a], first, count, n)
        packed.append(pieces)
        tops[a].append(top[:, 0, :])
    came = [send(pieces) for pieces in packed]

    top = jnp.concatenate(tops[0] + tops[1], axis=0)
    top = lax.dynamic_slice_in_dim(jnp.concatenate([top, top], axis=1), me * width, depth, axis=1)
    all_tops = send([top[:, k * width : (k + 1) * width] for k in range(n)])
    scale = functools.reduce(jnp.maximum, all_tops)
    ratio = jnp.stack(all_tops, axis=-1) / scale[:, :, None]
    ratios = (ratio[:experts], ratio[experts:])

    wholes = [None, None]
    for c, (a, first, count) in enumerate(chunks):
        wholes[a] = unpack(here, ratios[a], came[c], wholes[a], first, (experts, width, n * rows))
    finals = [jnp.swapaxes(whole, 1, 2) for whole in wholes]

    part_router = (router_weight * router_gain[:, None]).astype(jnp.bfloat16).T
    routers = join(here, send([part_router] * n))
    serve_router = lax.all_gather(routers, "owner", axis=0, tiled=True).T
    return (*finals, scale[:experts], scale[experts:], serve_router)


def shards(n, master_gate, master_up, router_weight, router_gain):
    experts, rows, depth = master_gate.shape
    if fits(n, experts, rows, depth):
        return fast_shards(n, (master_gate, master_up), router_weight, router_gain)
    return plain_shards(master_gate, master_up, router_weight, router_gain)


def fits(n, experts, rows, depth):
    return n > 1 and experts > 1 and rows % 128 == 0 and depth % (16 * n) == 0 and depth % 128 == 0


def solution(mesh):
    n = mesh.shape["rows"]
    step = placed(mesh, n)

    return step


def placed(mesh, n):
    return jax.shard_map(
        functools.partial(shards, n),
        mesh=mesh,
        in_specs=(
            P("owner", "rows", None),
            P("owner", "rows", None),
            P("rows", "owner"),
            P("rows"),
        ),
        out_specs=(
            P("owner", None, "rows"),
            P("owner", None, "rows"),
            P("owner", "rows"),
            P("owner", "rows"),
            P(),
        ),
        check_vma=False,
    )
```

```python
import functools

import jax
import jax.numpy as jnp
from jax import lax
from jax.experimental import pallas as pl
from jax.experimental.pallas import tpu as pltpu
from jax.sharding import PartitionSpec as P


SPAN = 252.0
LN2 = 0.6931471805599453
TINY = 1e-30


def plain_shards(master_gate, master_up, router_weight, router_gain):
    scale_gate, scale_up = lax.pmax(
        (jnp.max(jnp.abs(master_gate), axis=1), jnp.max(jnp.abs(master_up), axis=1)), "rows"
    )
    finals, scales = [], []
    for master, scale in ((master_gate, scale_gate), (master_up, scale_up)):
        narrow = (master / jnp.expand_dims(scale, 1)).astype(jnp.bfloat16)
        final = lax.all_to_all(narrow, "rows", split_axis=2, concat_axis=1, tiled=True)
        width = final.shape[2]
        finals.append(final)
        scales.append(lax.dynamic_slice_in_dim(scale, lax.axis_index("rows") * width, width, axis=1))
    part_router = (router_weight * router_gain[:, None]).astype(jnp.bfloat16)
    row_router = lax.all_gather(part_router, "rows", axis=0, tiled=True)
    serve_router = lax.all_gather(row_router, "owner", axis=1, tiled=True)
    return (*finals, *scales, serve_router)


def pack_body(n, me_ref, x_ref, *refs):
    pieces, top_ref, turned = refs[:n], refs[n], refs[n + 1]
    depth = turned.shape[0]
    width = depth // n
    for c in range(depth // 128):
        cols = slice(128 * c, 128 * (c + 1))
        x = x_ref[0, :, cols]
        size = jnp.abs(x)
        top = jnp.max(size, axis=0, keepdims=True)
        top_ref[0, :, cols] = top
        root = jnp.sqrt(size * (1.0 / jnp.maximum(top, TINY)))
        code = jnp.exp((SPAN * LN2) * root - (SPAN * LN2 / 2))
        code = jnp.where(x < 0, -code, code)
        turned[cols, :] = code.T.astype(jnp.bfloat16)
    for k in range(n):
        to = lax.rem(me_ref[0] + k, n)
        pieces[k][0] = turned[pl.ds(pl.multiple_of(to * width, width), width), :]


def pack(me, master, first, count, n):
    _, rows, depth = master.shape
    width = depth // n
    return pl.pallas_call(
        functools.partial(pack_body, n),
        grid_spec=pltpu.PrefetchScalarGridSpec(
            num_scalar_prefetch=1,
            grid=(count,),
            in_specs=[pl.BlockSpec((1, rows, depth), lambda e, me: (first + e, 0, 0))],
            out_specs=[pl.BlockSpec((1, width, rows), lambda e, me: (e, 0, 0))] * n
            + [pl.BlockSpec((1, 1, depth), lambda e, me: (e, 0, 0))],
            scratch_shapes=[pltpu.VMEM((depth, rows), jnp.bfloat16)],
        ),
        out_shape=[jax.ShapeDtypeStruct((count, width, rows), jnp.bfloat16)] * n
        + [jax.ShapeDtypeStruct((count, 1, depth), jnp.float32)],
        cost_estimate=pl.CostEstimate(
            flops=count * rows * depth * 40, bytes_accessed=count * rows * depth * 6, transcendentals=0
        ),
    )(me, master)


def unpack_body(n, first, start, me_ref, *refs):
    tops, pieces, out, ratios = refs[:n], refs[n : 2 * n], refs[-2], refs[-1]
    width, rows = pieces[0].shape[1:]
    step = 16
    expert = first + pl.program_id(0)
    top = jnp.concatenate([t[pl.ds(expert, 1), start : start + width] for t in tops], axis=0)
    ratios[...] = (top / jnp.max(top, axis=0, keepdims=True)).T

    def some_rows(i, _):
        part = pl.ds(pl.multiple_of(i * step, step), step)
        ratio = ratios[part, :]
        for k in range(n):
            code = pieces[k][0, part, :].astype(jnp.float32)
            root = jnp.log(jnp.abs(code)) * (1.0 / (SPAN * LN2)) + 0.5
            value = root * root * ratio[:, k : k + 1]
            value = jnp.where(code < 0, -value, value).astype(jnp.bfloat16)
            source = lax.rem(me_ref[0] + (n - k), n)
            out[0, part, pl.ds(pl.multiple_of(source * rows, rows), rows)] = value
        return 0

    lax.fori_loop(0, width // step, some_rows, 0)


def unpack(me, tops, start, pieces, whole, first, shape):
    n = len(pieces)
    count, width, rows = pieces[0].shape
    operands = [*tops, *pieces] + ([] if whole is None else [whole])
    return pl.pallas_call(
        functools.partial(unpack_body, n, first, start),
        grid_spec=pltpu.PrefetchScalarGridSpec(
            num_scalar_prefetch=1,
            grid=(count,),
            in_specs=[pl.BlockSpec(tops[0].shape, lambda e, me: (0, 0))] * n
            + [pl.BlockSpec((1, width, rows), lambda e, me: (e, 0, 0))] * n
            + ([] if whole is None else [pl.BlockSpec(memory_space=pl.ANY)]),
            out_specs=pl.BlockSpec((1, width, n * rows), lambda e, me: (first + e, 0, 0)),
            scratch_shapes=[pltpu.VMEM((width, n), jnp.float32)],
        ),
        out_shape=jax.ShapeDtypeStruct(shape, jnp.bfloat16),
        input_output_aliases={} if whole is None else {2 * n + 1: 0},
        cost_estimate=pl.CostEstimate(
            flops=count * rows * width * n * 30, bytes_accessed=count * rows * width * n * 4, transcendentals=0
        ),
    )(me, *operands)


def join_body(n, me_ref, *refs):
    out, half = refs[-1], n // 2
    columns, rows = refs[0].shape[0] // 2, refs[0].shape[1]
    place = lax.rem(me_ref[0], half)
    for k in range(half):
        source = me_ref[0] - place + lax.rem(place + (half - k), half)
        for part in range(2):
            at = lax.rem(source + part * half, n) * rows
            out[:, pl.ds(pl.multiple_of(at, rows), rows)] = refs[k][columns * part : columns * (part + 1), :]


def join(n, me, pairs):
    columns, rows = pairs[0].shape[0] // 2, pairs[0].shape[1]
    return pl.pallas_call(
        functools.partial(join_body, n),
        in_specs=[pl.BlockSpec(memory_space=pltpu.SMEM)] + [pl.BlockSpec(memory_space=pltpu.VMEM)] * len(pairs),
        out_specs=pl.BlockSpec(memory_space=pltpu.VMEM),
        out_shape=jax.ShapeDtypeStruct((columns, n * rows), jnp.bfloat16),
        name="join",
    )(me, *pairs)


def plan(experts):
    first = [c for c in (experts // 8, experts // 3) if c]
    last = [c for c in (experts // 4, experts // 8, experts // 16) if c]
    counts = ((*first, experts - sum(first)), (experts - sum(last), *last))
    return [(a, sum(counts[a][:c]), count) for a in range(2) for c, count in enumerate(counts[a])]


def send_order(n):
    return sorted(range(1, n), key=lambda k: abs(2 * k - n))


def fast_shards(n, masters, router_weight, router_gain):
    me = lax.axis_index("rows")
    here = jnp.reshape(me, (1,)).astype(jnp.int32)
    experts, rows, depth = masters[0].shape
    width = depth // n
    turns = [[(r, (r + k) % n) for r in range(n)] for k in range(n)]

    def send(pieces):
        came = list(pieces)
        for k in send_order(n):
            came[k] = lax.ppermute(pieces[k], "rows", turns[k])
        return came

    chunks = plan(experts)
    packed, tops = [], [[], []]
    for a, first, count in chunks:
        *pieces, top = pack(here, masters[a], first, count, n)
        packed.append(pieces)
        tops[a].append(top[:, 0, :])
    came = [send(pieces) for pieces in packed]

    tops = [jnp.concatenate(some, axis=0) for some in tops]
    tops = [lax.dynamic_slice_in_dim(jnp.concatenate([t, t], axis=1), me * width, depth, axis=1) for t in tops]
    tops = send([jnp.concatenate([t[:, k * width : (k + 1) * width] for t in tops], axis=1) for k in range(n)])
    scale = functools.reduce(jnp.maximum, tops)

    wholes = [None, None]
    for c, (a, first, count) in enumerate(chunks):
        wholes[a] = unpack(here, tops, a * width, came[c], wholes[a], first, (experts, width, n * rows))
    finals = [jnp.swapaxes(whole, 1, 2) for whole in wholes]

    half = n // 2
    router = (router_weight * router_gain[:, None]).astype(jnp.bfloat16).T
    pair = [router, lax.ppermute(router, "rows", turns[half])]
    pairs = [jnp.concatenate(pair, axis=0)]
    for k in range(1, half):
        inside = [(r, r // half * half + (r + k) % half) for r in range(n)]
        pairs.append(lax.ppermute(pairs[0], "rows", inside))
    serve_router = lax.all_gather(join(n, here, pairs), "owner", axis=0, tiled=True).T
    return (*finals, scale[:, :width], scale[:, width:], serve_router)


def shards(n, master_gate, master_up, router_weight, router_gain):
    experts, rows, depth = master_gate.shape
    if fits(n, experts, rows, depth):
        return fast_shards(n, (master_gate, master_up), router_weight, router_gain)
    return plain_shards(master_gate, master_up, router_weight, router_gain)


def fits(n, experts, rows, depth):
    return n % 2 == 0 and experts >= 8 and rows % 128 == 0 and depth % (16 * n) == 0 and depth % 128 == 0


def solution(mesh):
    n = mesh.shape["rows"]
    step = placed(mesh, n)

    return step


def placed(mesh, n):
    return jax.shard_map(
        functools.partial(shards, n),
        mesh=mesh,
        in_specs=(
            P("owner", "rows", None),
            P("owner", "rows", None),
            P("rows", "owner"),
            P("rows"),
        ),
        out_specs=(
            P("owner", None, "rows"),
            P("owner", None, "rows"),
            P("owner", "rows"),
            P("owner", "rows"),
            P(),
        ),
        check_vma=False,
    )
```

```python
import functools

import jax
import jax.numpy as jnp
from jax import lax
from jax.experimental import pallas as pl
from jax.experimental.pallas import tpu as pltpu
from jax.sharding import PartitionSpec as P


SPAN = 252.0
LN2 = 0.6931471805599453
TINY = 1e-30


def plain_shards(master_gate, master_up, router_weight, router_gain):
    scale_gate, scale_up = lax.pmax(
        (jnp.max(jnp.abs(master_gate), axis=1), jnp.max(jnp.abs(master_up), axis=1)), "rows"
    )
    finals, scales = [], []
    for master, scale in ((master_gate, scale_gate), (master_up, scale_up)):
        narrow = (master / jnp.expand_dims(scale, 1)).astype(jnp.bfloat16)
        final = lax.all_to_all(narrow, "rows", split_axis=2, concat_axis=1, tiled=True)
        width = final.shape[2]
        finals.append(final)
        scales.append(lax.dynamic_slice_in_dim(scale, lax.axis_index("rows") * width, width, axis=1))
    part_router = (router_weight * router_gain[:, None]).astype(jnp.bfloat16)
    row_router = lax.all_gather(part_router, "rows", axis=0, tiled=True)
    serve_router = lax.all_gather(row_router, "owner", axis=1, tiled=True)
    return (*finals, *scales, serve_router)


def pack_body(n, me_ref, x_ref, *refs):
    pieces, top_ref, turned = refs[:n], refs[n], refs[n + 1]
    depth = turned.shape[0]
    width = depth // n
    for c in range(depth // 128):
        cols = slice(128 * c, 128 * (c + 1))
        x = x_ref[0, :, cols]
        size = jnp.abs(x)
        top = jnp.max(size, axis=0, keepdims=True)
        top_ref[0, :, cols] = top
        square = size * (SPAN * SPAN / jnp.maximum(top, TINY))
        root = square * lax.rsqrt(jnp.maximum(square, TINY))
        code = jnp.exp2(root - SPAN / 2)
        turned[cols, :] = jnp.where(x < 0, -code, code).T
    for k in range(n):
        to = lax.rem(me_ref[0] + k, n)
        pieces[k][0] = turned[pl.ds(pl.multiple_of(to * width, width), width), :].astype(jnp.bfloat16)


def pack(me, master, first, count, n):
    _, rows, depth = master.shape
    width = depth // n
    return pl.pallas_call(
        functools.partial(pack_body, n),
        grid_spec=pltpu.PrefetchScalarGridSpec(
            num_scalar_prefetch=1,
            grid=(count,),
            in_specs=[pl.BlockSpec((1, rows, depth), lambda e, me: (first + e, 0, 0))],
            out_specs=[pl.BlockSpec((1, width, rows), lambda e, me: (e, 0, 0))] * n
            + [pl.BlockSpec((1, 1, depth), lambda e, me: (e, 0, 0))],
            scratch_shapes=[pltpu.VMEM((depth, rows), jnp.float32)],
        ),
        out_shape=[jax.ShapeDtypeStruct((count, width, rows), jnp.bfloat16)] * n
        + [jax.ShapeDtypeStruct((count, 1, depth), jnp.float32)],
        cost_estimate=pl.CostEstimate(
            flops=count * rows * depth * 40, bytes_accessed=count * rows * depth * 6, transcendentals=0
        ),
    )(me, master)


def unpack_body(n, first, start, me_ref, *refs):
    tops, pieces, out, ratios = refs[:n], refs[n : 2 * n], refs[-2], refs[-1]
    width, rows = pieces[0].shape[1:]
    step = 16
    expert = first + pl.program_id(0)
    top = jnp.concatenate([t[pl.ds(expert, 1), start : start + width] for t in tops], axis=0)
    ratios[...] = (top / jnp.max(top, axis=0, keepdims=True)).T

    for i in range(width // step):
        part = slice(i * step, (i + 1) * step)
        ratio = ratios[part, :]
        for k in range(n):
            code = pieces[k][0, part, :].astype(jnp.float32)
            root = jnp.log(jnp.abs(code)) * (1.0 / (SPAN * LN2)) + 0.5
            up = ratio[:, k : k + 1]
            value = root * root * jnp.where(code < 0, -up, up)
            source = lax.rem(me_ref[0] + (n - k), n)
            out[0, part, pl.ds(pl.multiple_of(source * rows, rows), rows)] = value.astype(jnp.bfloat16)


def unpack(me, tops, start, pieces, whole, first, shape):
    n = len(pieces)
    count, width, rows = pieces[0].shape
    operands = [*tops, *pieces] + ([] if whole is None else [whole])
    return pl.pallas_call(
        functools.partial(unpack_body, n, first, start),
        grid_spec=pltpu.PrefetchScalarGridSpec(
            num_scalar_prefetch=1,
            grid=(count,),
            in_specs=[pl.BlockSpec(tops[0].shape, lambda e, me: (0, 0))] * n
            + [pl.BlockSpec((1, width, rows), lambda e, me: (e, 0, 0))] * n
            + ([] if whole is None else [pl.BlockSpec(memory_space=pl.ANY)]),
            out_specs=pl.BlockSpec((1, width, n * rows), lambda e, me: (first + e, 0, 0)),
            scratch_shapes=[pltpu.VMEM((width, n), jnp.float32)],
        ),
        out_shape=jax.ShapeDtypeStruct(shape, jnp.bfloat16),
        input_output_aliases={} if whole is None else {2 * n + 1: 0},
        cost_estimate=pl.CostEstimate(
            flops=count * rows * width * n * 30, bytes_accessed=count * rows * width * n * 4, transcendentals=0
        ),
    )(me, *operands)


def join_body(n, me_ref, gathered, out):
    half = n // 2
    rows = gathered.shape[1]
    columns = out.shape[0]
    place = lax.rem(me_ref[0], half)
    for k in range(half):
        source = me_ref[0] - place + lax.rem(place + (half - k), half)
        for part in range(2):
            at = lax.rem(source + part * half, n) * rows
            here = slice((2 * k + part) * columns, (2 * k + part + 1) * columns)
            out[:, pl.ds(pl.multiple_of(at, rows), rows)] = gathered[here, :]


def join(n, me, gathered, owners):
    rows = gathered.shape[1]
    columns = gathered.shape[0] // (owners * n)
    return pl.pallas_call(
        functools.partial(join_body, n),
        grid_spec=pltpu.PrefetchScalarGridSpec(
            num_scalar_prefetch=1,
            grid=(owners,),
            in_specs=[pl.BlockSpec((n * columns, rows), lambda o, me: (o, 0))],
            out_specs=pl.BlockSpec((columns, n * rows), lambda o, me: (o, 0)),
        ),
        out_shape=jax.ShapeDtypeStruct((owners * columns, n * rows), jnp.bfloat16),
        name="join",
    )(me, gathered)


def plan(experts):
    first = [c for c in (experts // 8, experts // 3) if c]
    last = [c for c in (experts // 4, experts // 8, experts // 16) if c]
    counts = ((*first, experts - sum(first)), (experts - sum(last), *last))
    return [(a, sum(counts[a][:c]), count) for a in range(2) for c, count in enumerate(counts[a])]


def send_order(n):
    return sorted(range(1, n), key=lambda k: abs(2 * k - n))


def fast_shards(n, masters, router_weight, router_gain):
    me = lax.axis_index("rows")
    here = jnp.reshape(me, (1,)).astype(jnp.int32)
    experts, rows, depth = masters[0].shape
    width = depth // n
    turns = [[(r, (r + k) % n) for r in range(n)] for k in range(n)]

    def send(pieces):
        came = list(pieces)
        for k in send_order(n):
            came[k] = lax.ppermute(pieces[k], "rows", turns[k])
        return came

    chunks = plan(experts)
    packed, tops = [], [[], []]
    for a, first, count in chunks:
        *pieces, top = pack(here, masters[a], first, count, n)
        packed.append(pieces)
        tops[a].append(top[:, 0, :])
    came = [send(pieces) for pieces in packed]

    tops = [jnp.concatenate(some, axis=0) for some in tops]
    tops = [lax.dynamic_slice_in_dim(jnp.concatenate([t, t], axis=1), me * width, depth, axis=1) for t in tops]
    tops = send([jnp.concatenate([t[:, k * width : (k + 1) * width] for t in tops], axis=1) for k in range(n)])
    scale = functools.reduce(jnp.maximum, tops)

    wholes = [None, None]
    for c, (a, first, count) in enumerate(chunks):
        wholes[a] = unpack(here, tops, a * width, came[c], wholes[a], first, (experts, width, n * rows))
    finals = [jnp.swapaxes(whole, 1, 2) for whole in wholes]

    half = n // 2
    router = (router_weight * router_gain[:, None]).astype(jnp.bfloat16).T
    pair = [router, lax.ppermute(router, "rows", turns[half])]
    pairs = [jnp.concatenate(pair, axis=0)]
    for k in range(1, half):
        inside = [(r, r // half * half + (r + k) % half) for r in range(n)]
        pairs.append(lax.ppermute(pairs[0], "rows", inside))
    gathered = lax.all_gather(jnp.concatenate(pairs, axis=0), "owner", axis=0, tiled=True)
    serve_router = join(n, here, gathered, gathered.shape[0] // pairs[0].shape[0] // half).T
    return (*finals, scale[:, :width], scale[:, width:], serve_router)


def shards(n, master_gate, master_up, router_weight, router_gain):
    experts, rows, depth = master_gate.shape
    if fits(n, experts, rows, depth):
        return fast_shards(n, (master_gate, master_up), router_weight, router_gain)
    return plain_shards(master_gate, master_up, router_weight, router_gain)


def fits(n, experts, rows, depth):
    return n % 2 == 0 and experts >= 8 and rows % 128 == 0 and depth % (16 * n) == 0 and depth % 128 == 0


def solution(mesh):
    n = mesh.shape["rows"]
    step = placed(mesh, n)

    return step


def placed(mesh, n):
    return jax.shard_map(
        functools.partial(shards, n),
        mesh=mesh,
        in_specs=(
            P("owner", "rows", None),
            P("owner", "rows", None),
            P("rows", "owner"),
            P("rows"),
        ),
        out_specs=(
            P("owner", None, "rows"),
            P("owner", None, "rows"),
            P("owner", "rows"),
            P("owner", "rows"),
            P(),
        ),
        check_vma=False,
    )
```

```python
import functools

import jax
import jax.numpy as jnp
from jax import lax
from jax.experimental import pallas as pl
from jax.experimental.pallas import tpu as pltpu
from jax.sharding import PartitionSpec as P


SPAN = 252.0
LN2 = 0.6931471805599453
TINY = 1e-30


def plain_shards(master_gate, master_up, router_weight, router_gain):
    scale_gate, scale_up = lax.pmax(
        (jnp.max(jnp.abs(master_gate), axis=1), jnp.max(jnp.abs(master_up), axis=1)), "rows"
    )
    finals, scales = [], []
    for master, scale in ((master_gate, scale_gate), (master_up, scale_up)):
        narrow = (master / jnp.expand_dims(scale, 1)).astype(jnp.bfloat16)
        final = lax.all_to_all(narrow, "rows", split_axis=2, concat_axis=1, tiled=True)
        width = final.shape[2]
        finals.append(final)
        scales.append(lax.dynamic_slice_in_dim(scale, lax.axis_index("rows") * width, width, axis=1))
    part_router = (router_weight * router_gain[:, None]).astype(jnp.bfloat16)
    row_router = lax.all_gather(part_router, "rows", axis=0, tiled=True)
    serve_router = lax.all_gather(row_router, "owner", axis=1, tiled=True)
    return (*finals, *scales, serve_router)


def coded(x):
    size = jnp.abs(x)
    top = jnp.max(size, axis=0, keepdims=True)
    square = size * (SPAN * SPAN / jnp.maximum(top, TINY))
    root = square * lax.rsqrt(jnp.maximum(square, TINY))
    code = jnp.exp2(root - SPAN / 2)
    return jnp.where(x < 0, -code, code), top


def pack_body(n, me_ref, x_ref, *refs):
    pieces, top_ref, turned = refs[:n], refs[n], refs[n + 1]
    depth = turned.shape[0]
    width = depth // n
    for c in range(depth // 128):
        cols = slice(128 * c, 128 * (c + 1))
        code, top_ref[0, :, cols] = coded(x_ref[0, :, cols])
        turned[cols, :] = code.T
    for k in range(n):
        to = lax.rem(me_ref[0] + k, n)
        pieces[k][0] = turned[pl.ds(pl.multiple_of(to * width, width), width), :].astype(jnp.bfloat16)


def window(n, me, depth, tiles):
    column = lax.rem(me + n // 2, n) * (depth // n)
    return column, jnp.minimum(lax.div(column, 128), depth // 128 - tiles)


def lead_body(n, depth, me_ref, *refs):
    tiles, piece, turned = refs[:-2], refs[-2], refs[-1]
    column, tile = window(n, me_ref[0], depth, len(tiles))
    width = depth // n
    at = pl.multiple_of(column - tile * 128, 16)
    for e in range(piece.shape[0]):
        for c, part in enumerate(tiles):
            turned[e, 128 * c : 128 * (c + 1), :] = coded(part[e])[0].T
        piece[e] = turned[e, pl.ds(at, width), :].astype(jnp.bfloat16)


def lead(me, master, first, count, n):
    _, rows, depth = master.shape
    width = depth // n
    tiles = min((width - 16) // 128 + 2, depth // 128)
    spec = lambda c: pl.BlockSpec(
        (count, rows, 128), lambda e, me: (first // count, 0, window(n, me[0], depth, tiles)[1] + c)
    )
    return pl.pallas_call(
        functools.partial(lead_body, n, depth),
        grid_spec=pltpu.PrefetchScalarGridSpec(
            num_scalar_prefetch=1,
            grid=(1,),
            in_specs=[spec(c) for c in range(tiles)],
            out_specs=pl.BlockSpec((count, width, rows), lambda e, me: (0, 0, 0)),
            scratch_shapes=[pltpu.VMEM((count, tiles * 128, rows), jnp.float32)],
        ),
        out_shape=jax.ShapeDtypeStruct((count, width, rows), jnp.bfloat16),
        cost_estimate=pl.CostEstimate(
            flops=count * rows * width * 40, bytes_accessed=count * rows * width * 8, transcendentals=0
        ),
        name="lead",
    )(me, *[master] * tiles)


def pack(me, master, first, count, n):
    _, rows, depth = master.shape
    width = depth // n
    return pl.pallas_call(
        functools.partial(pack_body, n),
        grid_spec=pltpu.PrefetchScalarGridSpec(
            num_scalar_prefetch=1,
            grid=(count,),
            in_specs=[pl.BlockSpec((1, rows, depth), lambda e, me: (first + e, 0, 0))],
            out_specs=[pl.BlockSpec((1, width, rows), lambda e, me: (e, 0, 0))] * n
            + [pl.BlockSpec((1, 1, depth), lambda e, me: (e, 0, 0))],
            scratch_shapes=[pltpu.VMEM((depth, rows), jnp.float32)],
        ),
        out_shape=[jax.ShapeDtypeStruct((count, width, rows), jnp.bfloat16)] * n
        + [jax.ShapeDtypeStruct((count, 1, depth), jnp.float32)],
        cost_estimate=pl.CostEstimate(
            flops=count * rows * depth * 40, bytes_accessed=count * rows * depth * 6, transcendentals=0
        ),
    )(me, master)


def ratios_of(tops, expert, start, width):
    top = jnp.concatenate([t[pl.ds(expert, 1), start : start + width] for t in tops], axis=0)
    return (top / jnp.max(top, axis=0, keepdims=True)).T


def decoded(code, up):
    code = code.astype(jnp.float32)
    root = jnp.log(jnp.abs(code)) * (1.0 / (SPAN * LN2)) + 0.5
    return (root * root * jnp.where(code < 0, -up, up)).astype(jnp.bfloat16)


def unpack_body(n, first, start, me_ref, *refs):
    tops, pieces, out, ratios = refs[:n], refs[n : 2 * n], refs[-2], refs[-1]
    width, rows = pieces[0].shape[1:]
    step = 16
    ratios[...] = ratios_of(tops, first + pl.program_id(0), start, width)
    for i in range(width // step):
        part = slice(i * step, (i + 1) * step)
        ratio = ratios[part, :]
        for k in range(n):
            source = lax.rem(me_ref[0] + (n - k), n)
            lanes = pl.ds(pl.multiple_of(source * rows, rows), rows)
            out[0, part, lanes] = decoded(pieces[k][0, part, :], ratio[:, k : k + 1])


def unpack_some_body(n, sources, first, start, me_ref, *refs):
    m = len(sources)
    tops, pieces = refs[:n], refs[n : n + m]
    out, done, ratios, sems = refs[-4:]
    count, width, rows = pieces[0].shape
    step = 16
    for e in range(count):
        ratios[e] = ratios_of(tops, first + e, start, width)
    copies = []
    for p, k in enumerate(sources):
        for e in range(count):
            for i in range(width // step):
                part = slice(i * step, (i + 1) * step)
                done[p, e, part, :] = decoded(pieces[p][e, part, :], ratios[e, part, k : k + 1])
        lane = pl.multiple_of(lax.rem(me_ref[0] + (n - k), n) * rows, rows)
        target = out.at[pl.ds(first, count), :, pl.ds(lane, rows)]
        copies.append(pltpu.make_async_copy(done.at[p], target, sems.at[p]))
        copies[-1].start()
    for copy in copies:
        copy.wait()


def unpack_some(me, tops, start, pieces, sources, whole, first):
    n, m = len(tops), len(sources)
    count, width, rows = pieces[0].shape
    return pl.pallas_call(
        functools.partial(unpack_some_body, n, sources, first, start),
        grid_spec=pltpu.PrefetchScalarGridSpec(
            num_scalar_prefetch=1,
            grid=(1,),
            in_specs=[pl.BlockSpec(tops[0].shape, lambda e, me: (0, 0))] * n
            + [pl.BlockSpec((count, width, rows), lambda e, me: (0, 0, 0))] * m
            + [pl.BlockSpec(memory_space=pl.ANY)],
            out_specs=pl.BlockSpec(memory_space=pl.ANY),
            scratch_shapes=[
                pltpu.VMEM((m, count, width, rows), jnp.bfloat16),
                pltpu.VMEM((count, width, n), jnp.float32),
                pltpu.SemaphoreType.DMA((m,)),
            ],
        ),
        out_shape=jax.ShapeDtypeStruct(whole.shape, jnp.bfloat16),
        input_output_aliases={n + m + 1: 0},
        cost_estimate=pl.CostEstimate(
            flops=count * rows * width * m * 30, bytes_accessed=count * rows * width * m * 4, transcendentals=0
        ),
    )(me, *tops, *pieces, whole)


def unpack(me, tops, start, pieces, whole, first, shape):
    n = len(pieces)
    count, width, rows = pieces[0].shape
    operands = [*tops, *pieces] + ([] if whole is None else [whole])
    return pl.pallas_call(
        functools.partial(unpack_body, n, first, start),
        grid_spec=pltpu.PrefetchScalarGridSpec(
            num_scalar_prefetch=1,
            grid=(count,),
            in_specs=[pl.BlockSpec(tops[0].shape, lambda e, me: (0, 0))] * n
            + [pl.BlockSpec((1, width, rows), lambda e, me: (e, 0, 0))] * n
            + ([] if whole is None else [pl.BlockSpec(memory_space=pl.ANY)]),
            out_specs=pl.BlockSpec((1, width, n * rows), lambda e, me: (first + e, 0, 0)),
            scratch_shapes=[pltpu.VMEM((width, n), jnp.float32)],
        ),
        out_shape=jax.ShapeDtypeStruct(shape, jnp.bfloat16),
        input_output_aliases={} if whole is None else {2 * n + 1: 0},
        cost_estimate=pl.CostEstimate(
            flops=count * rows * width * n * 30, bytes_accessed=count * rows * width * n * 4, transcendentals=0
        ),
    )(me, *operands)


def join_body(n, me_ref, gathered, out):
    half = n // 2
    rows = gathered.shape[1]
    columns = out.shape[0]
    place = lax.rem(me_ref[0], half)
    for k in range(half):
        source = me_ref[0] - place + lax.rem(place + (half - k), half)
        for part in range(2):
            at = lax.rem(source + part * half, n) * rows
            here = slice((2 * k + part) * columns, (2 * k + part + 1) * columns)
            out[:, pl.ds(pl.multiple_of(at, rows), rows)] = gathered[here, :]


def join(n, me, gathered, owners):
    rows = gathered.shape[1]
    columns = gathered.shape[0] // (owners * n)
    return pl.pallas_call(
        functools.partial(join_body, n),
        grid_spec=pltpu.PrefetchScalarGridSpec(
            num_scalar_prefetch=1,
            grid=(owners,),
            in_specs=[pl.BlockSpec((n * columns, rows), lambda o, me: (o, 0))],
            out_specs=pl.BlockSpec((columns, n * rows), lambda o, me: (o, 0)),
        ),
        out_shape=jax.ShapeDtypeStruct((owners * columns, n * rows), jnp.bfloat16),
        name="join",
    )(me, gathered)


def plan(experts):
    first = (3 * experts // 16, experts // 3)
    counts = ((*first, experts - sum(first)), (experts - experts // 4, experts // 4))
    return [(a, sum(counts[a][:c]), count) for a in range(2) for c, count in enumerate(counts[a])]


def send_order(n):
    return sorted(range(1, n), key=lambda k: abs(2 * k - n))


def last_groups(n):
    line = [0, *send_order(n)]
    return (line[: n // 2], line[n // 2 :])


def fast_shards(n, masters, router_weight, router_gain):
    me = lax.axis_index("rows")
    here = jnp.reshape(me, (1,)).astype(jnp.int32)
    experts, rows, depth = masters[0].shape
    width = depth // n
    turns = [[(r, (r + k) % n) for r in range(n)] for k in range(n)]

    def send(pieces):
        came = list(pieces)
        for k in send_order(n):
            came[k] = lax.ppermute(pieces[k], "rows", turns[k])
        return came

    chunks = plan(experts)
    packed, tops = [], [[], []]
    for c, (a, first, count) in enumerate(chunks):
        *pieces, top = pack(here, masters[a], first, count, n)
        if c == 0:
            pieces[n // 2] = lead(here, masters[a], first, count, n)
        packed.append(pieces)
        tops[a].append(top[:, 0, :])
    came = [send(pieces) for pieces in packed]

    tops = [jnp.concatenate(some, axis=0) for some in tops]
    tops = [lax.dynamic_slice_in_dim(jnp.concatenate([t, t], axis=1), me * width, depth, axis=1) for t in tops]
    tops = send([jnp.concatenate([t[:, k * width : (k + 1) * width] for t in tops], axis=1) for k in range(n)])
    scale = functools.reduce(jnp.maximum, tops)

    wholes = [None, None]
    for c, (a, first, count) in enumerate(chunks):
        if c == len(chunks) - 1:
            for sources in last_groups(n):
                pieces = [came[c][k] for k in sources]
                wholes[a] = unpack_some(here, tops, a * width, pieces, sources, wholes[a], first)
            break
        wholes[a] = unpack(here, tops, a * width, came[c], wholes[a], first, (experts, width, n * rows))
    finals = [jnp.swapaxes(whole, 1, 2) for whole in wholes]

    half = n // 2
    router = (router_weight * router_gain[:, None]).astype(jnp.bfloat16).T
    pair = [router, lax.ppermute(router, "rows", turns[half])]
    pairs = [jnp.concatenate(pair, axis=0)]
    for k in range(1, half):
        inside = [(r, r // half * half + (r + k) % half) for r in range(n)]
        pairs.append(lax.ppermute(pairs[0], "rows", inside))
    gathered = lax.all_gather(jnp.concatenate(pairs, axis=0), "owner", axis=0, tiled=True)
    serve_router = join(n, here, gathered, gathered.shape[0] // pairs[0].shape[0] // half).T
    return (*finals, scale[:, :width], scale[:, width:], serve_router)


def shards(n, master_gate, master_up, router_weight, router_gain):
    experts, rows, depth = master_gate.shape
    if fits(n, experts, rows, depth):
        return fast_shards(n, (master_gate, master_up), router_weight, router_gain)
    return plain_shards(master_gate, master_up, router_weight, router_gain)


def fits(n, experts, rows, depth):
    return n % 2 == 0 and experts % 4 == 0 and experts >= 8 and rows % 128 == 0 and depth % (16 * n) == 0 and depth % 128 == 0


def solution(mesh):
    n = mesh.shape["rows"]
    step = placed(mesh, n)

    return step


def placed(mesh, n):
    return jax.shard_map(
        functools.partial(shards, n),
        mesh=mesh,
        in_specs=(
            P("owner", "rows", None),
            P("owner", "rows", None),
            P("rows", "owner"),
            P("rows"),
        ),
        out_specs=(
            P("owner", None, "rows"),
            P("owner", None, "rows"),
            P("owner", "rows"),
            P("owner", "rows"),
            P(),
        ),
        check_vma=False,
    )
```
